32 devices in a mesh: rep: 4 (over y, core), row: 4 (over z), col: 2 (over x).
Axes of the slice: x: 2, y: 2, z: 4, core: 2. Of those that a mesh axis runs over, the one named last changes fastest.
Arguments:
- patches: bfloat16 [4096, 588], P(('rep', 'col')), may hold values from -20 to 20
- embed_weight: bfloat16 [588, 6144], P(None, 'row'), may hold values from -1 to 1
- embed_bias: float32 [6144], P('row'), may hold values from -3 to 3
- old_in: bfloat16 [64, 768, 1536], P(('row', 'col')), may hold values from -0.078125 to 0.078125
- old_out: bfloat16 [64, 1536, 768], P(('row', 'col')), may hold values from -0.0546875 to 0.0546875
- restore_id: int32 [1], replicated, may hold values from 0 to 47
- norm_gains: float32 [48, 6144], P(None, 'row'), may hold values from 0.1 to 1.9
- in_biases: float32 [48, 12288], P(None, 'col'), may hold values from -3 to 3
- out_biases: float32 [48, 6144], P(None, 'row'), may hold values from -3 to 3
- final_gain: float32 [6144], P('row'), may hold values from 0.1 to 1.9
- check_weight: bfloat16 [6144, 128], P('row'), may hold values from -0.078125 to 0.078125
Outputs:
- in_weight: bfloat16 [6144, 12288], P('row', 'col')
- out_weight: bfloat16 [12288, 6144], P('col', 'row')
- check_logits: float32 [4096, 128], P(('rep', 'col'))
The draws below stay inside these ranges and needn't reach their ends.
All inputs are finite; a program needn't handle non-finite values.
Results may differ from the reference program's by a relative error of at most 0.0062.
Values may be sent and summed in bfloat16 or wider, within the bound.
A program may use at most 192 MiB of HBM per device.

```python
import math
import jax
import jax.numpy as jnp
from jax import lax

D = 6144
PATCH = 588
LAYERS_ALL = 48
FF = 12288
OLD_GRID = 8
CHECK = 128
TOKENS = 4096


def draw_patches(key, part):
    base_key, scale_key = jax.random.split(key, 2)
    row_scale = jnp.exp(jax.random.uniform(scale_key, (TOKENS, 1), jnp.float32, math.log(0.5), math.log(5.0)))
    noise_part = jax.random.truncated_normal(base_key, -4.0, 4.0, (TOKENS, PATCH), jnp.float32)
    values = row_scale * noise_part
    return values.astype(jnp.bfloat16)


def draw_embed_weight(key, part):
    entry_key, column_key = jax.random.split(key, 2)
    position = jnp.arange(D, dtype=jnp.float32) / D
    trend_part = math.log(3.0) * (position - 0.5)
    jitter = jax.random.uniform(column_key, (D,), jnp.float32, -1.15, 1.15)
    entries = jax.random.truncated_normal(entry_key, -4.0, 4.0, (PATCH, D), jnp.float32)
    column_scale = jnp.exp(trend_part + jitter)
    return (entries * column_scale[None, :] / math.sqrt(PATCH)).astype(jnp.bfloat16)


def block_levels(key, extent, cuts, smallest, largest):
    factor_of, own = 1.0, jax.random.fold_in(key, 6)
    for dim, parts in cuts:
        draws = jnp.exp(jax.random.uniform(jax.random.fold_in(own, dim), (parts,), jnp.float32, smallest / len(cuts), largest / len(cuts)))
        factor_of = factor_of * jnp.repeat(draws, extent[dim] // parts).reshape([-1 if axis == dim else 1 for axis in range(len(extent))])
    return factor_of


def normal_values(rng, extent, deviation, reach, cuts=(), held_as=jnp.bfloat16):
    values = jax.random.normal(rng, extent, jnp.float32) * deviation
    if len(cuts) > 0:
        values = block_levels(rng, extent, cuts, -0.22, 0.18) * values
    return jnp.clip(values, min=-reach, max=reach).astype(held_as)


def setup_inputs(seed: int = 0) -> dict:
    key_of = jax.random.split(jax.random.key(seed), 12)
    return {
        "patches": draw_patches(jax.random.fold_in(key_of[11], 71), 0),
        "embed_weight": draw_embed_weight(jax.random.fold_in(key_of[11], 71), 0),
        "embed_bias": normal_values(key_of[2], (D,), 0.5, 3.0, ((0, 4),), jnp.float32),
        "old_in": normal_values(key_of[3], (OLD_GRID * OLD_GRID, D // OLD_GRID, FF // OLD_GRID), D ** -0.5, 0.078125, ((0, 8),)),
        "old_out": normal_values(key_of[4], (OLD_GRID * OLD_GRID, FF // OLD_GRID, D // OLD_GRID), FF ** -0.5, 0.0546875, ((0, 8),)),
        "restore_id": jax.random.randint(key_of[5], (1,), 0, LAYERS_ALL).astype(jnp.int32),
        "norm_gains": jnp.clip(1.0 + 0.18 * jax.random.normal(key_of[6], (LAYERS_ALL, D), jnp.float32), 0.1, 1.9),
        "in_biases": normal_values(key_of[7], (LAYERS_ALL, FF), 0.5, 3.0, ((1, 2),), jnp.float32),
        "out_biases": normal_values(key_of[8], (LAYERS_ALL, D), 0.5, 3.0, ((1, 4),), jnp.float32),
        "final_gain": jnp.clip(1.0 + 0.18 * jax.random.normal(key_of[9], (D,), jnp.float32), 0.1, 1.9),
        "check_weight": normal_values(key_of[10], (D, CHECK), D ** -0.5, 0.078125, ((0, 4),)),
    }


EPSILON = 1e-06

def assemble_in(old_tiles):
    tile_grid = old_tiles.reshape(OLD_GRID, OLD_GRID, D // OLD_GRID, FF // OLD_GRID)
    return tile_grid.transpose(0, 2, 1, 3).reshape(D, FF)

def assemble_out(old_tiles):
    tile_grid = old_tiles.reshape(OLD_GRID, OLD_GRID, FF // OLD_GRID, D // OLD_GRID)
    return tile_grid.transpose(1, 2, 0, 3).reshape(FF, D)

def pick_rows(restore_id, param_table):
    selector = (jnp.arange(param_table.shape[0], dtype=jnp.int32)[None, :] == restore_id[:, None]).astype(jnp.float32)
    return jnp.dot(selector, param_table, precision=lax.Precision.HIGHEST)[0]

def norm_rows(values, gain_row):
    feature_count = values.shape[1]
    average = lax.optimization_barrier(jnp.sum(values, axis=1, keepdims=True)) / feature_count
    square_mean = lax.optimization_barrier(jnp.sum(values * values, axis=1, keepdims=True)) / feature_count
    inverse_scale = lax.rsqrt(square_mean - average * average + EPSILON)
    return ((values - average) * inverse_scale * gain_row).astype(jnp.bfloat16)

def reference(patches, embed_weight, embed_bias, old_in, old_out, restore_id, norm_gains, in_biases, out_biases, final_gain, check_weight):
    in_weight = assemble_in(old_in)
    out_weight = assemble_out(old_out)
    layer_gain = pick_rows(restore_id, norm_gains)
    layer_in_bias = pick_rows(restore_id, in_biases)
    layer_out_bias = pick_rows(restore_id, out_biases)
    embedded = jnp.dot(patches, embed_weight, preferred_element_type=jnp.float32) + embed_bias
    normed = norm_rows(embedded, layer_gain)
    pre = jnp.dot(normed, in_weight, preferred_element_type=jnp.float32) + layer_in_bias
    hidden = jax.nn.gelu(pre, approximate=False).astype(jnp.bfloat16)
    updated = embedded + jnp.dot(hidden, out_weight, preferred_element_type=jnp.float32) + layer_out_bias
    final_normed = norm_rows(updated, final_gain)
    check_logits = jnp.dot(final_normed, check_weight, preferred_element_type=jnp.float32)
    return (in_weight, out_weight, check_logits)
```

```python
import jax
import jax.numpy as jnp
from jax import lax
from jax.sharding import PartitionSpec as P

EPSILON = 1e-06
CHUNKS = 2


def for_sending(shard):
    return jax.tree.map(lambda a: a.astype(jnp.bfloat16) if a.dtype == jnp.float32 else a, shard)


def partner(value, axis, bit):
    mask = 2**bit
    pairs = [(source, source ^ mask) for source in range(lax.axis_size(axis))]
    return lax.ppermute(value, axis, pairs)


def pick_rows(restore_id, param_table):
    selector = (
        jnp.arange(param_table.shape[0], dtype=jnp.int32)[None, :] == restore_id[:, None]
    ).astype(jnp.float32)
    return jnp.dot(selector, param_table, precision=lax.Precision.HIGHEST)[0]


def norm_rows(values, gain_row):
    feature_count = values.shape[1] * lax.axis_size("row")
    totals = lax.psum((jnp.sum(values, axis=1), jnp.sum(values * values, axis=1)), "row")
    average = totals[0][:, None] / feature_count
    spread = totals[1][:, None] / feature_count - average * average
    return ((values - average) * lax.rsqrt(spread + EPSILON) * gain_row).astype(jnp.bfloat16)


def move_halves(pieces, bit_total, device_index, exchange):
    for bit_number in range(bit_total):
        upper_side = device_index >> bit_number & 1 == 1
        outgoing = tuple(
            (jnp.where(upper_side, lower_part, upper_part) for lower_part, upper_part in pieces)
        )
        incoming = exchange(outgoing, bit_number)
        pieces = tuple(
            (
                (
                    jnp.where(upper_side, arrived, lower_part),
                    jnp.where(upper_side, upper_part, arrived),
                )
                for (lower_part, upper_part), arrived in zip(pieces, incoming)
            )
        )
    return pieces


def butterfly_weights(old_in, old_out):
    tiles_here, tile_rows, tile_cols = old_in.shape
    local_cols = tiles_here * tile_cols
    half_cols = local_cols // 2
    in_local = jnp.transpose(old_in, (1, 0, 2)).reshape(tile_rows, local_cols)
    out_local = old_out.reshape(local_cols, tile_rows)
    col_index = lax.axis_index("col")
    col_count = lax.axis_size("col")
    col_bits = col_count.bit_length() - 1
    pieces = (
        (in_local[:, :half_cols], in_local[:, half_cols:]),
        (out_local[:half_cols], out_local[half_cols:]),
    )
    pieces = move_halves(
        pieces,
        col_bits,
        col_index,
        lambda send_parts, bit_number: jax.tree.map(
            lambda part, own: part.astype(own.dtype),
            partner(for_sending(send_parts), "col", bit_number),
            send_parts,
        ),
    )
    in_pair, out_pair = pieces
    in_weight = jnp.concatenate(in_pair, axis=0)
    out_weight = jnp.concatenate(out_pair, axis=1)
    return in_weight, out_weight


def shared_exchange(old_in, old_out):
    tiles_here, tile_rows, tile_cols = old_in.shape
    half_tiles = tiles_here // 2
    half_cols = half_tiles * tile_cols
    col_index = lax.axis_index("col")
    rep_index = lax.axis_index("rep")
    rep_count = lax.axis_size("rep")
    in_parts = old_in.reshape(2, rep_count, half_tiles * tile_rows // rep_count, tile_cols)
    share = lax.dynamic_slice(
        in_parts, (1 - col_index, rep_index, 0, 0), (1, 1) + in_parts.shape[2:]
    )[0, 0]
    share = partner(share, "col", 0)
    out_parts = old_out.reshape(2, half_cols, tile_rows)
    out_sent = lax.dynamic_index_in_dim(out_parts, 1 - col_index, 0, keepdims=False)
    out_kept = lax.dynamic_index_in_dim(out_parts, col_index, 0, keepdims=False)
    share, out_sent = lax.optimization_barrier((share, out_sent))
    out_arrived = partner(out_sent, "col", 0)
    in_arrived = lax.all_gather(share, "rep", axis=0, tiled=True)

    def as_rows(tiles):
        rows = tiles.reshape(half_tiles, tile_rows, tile_cols)
        return jnp.transpose(rows, (1, 0, 2)).reshape(1, tile_rows, half_cols)

    kept = as_rows(lax.dynamic_index_in_dim(in_parts, col_index, 0, keepdims=False))
    blocks = jnp.zeros((2, tile_rows, half_cols), old_in.dtype)
    blocks = lax.dynamic_update_slice(blocks, kept, (col_index, 0, 0))
    blocks = lax.dynamic_update_slice(blocks, as_rows(in_arrived), (1 - col_index, 0, 0))
    return blocks.reshape(2 * tile_rows, half_cols), out_kept, out_arrived


def join_out(out_kept, out_arrived):
    upper_side = lax.axis_index("col") == 1
    return jnp.concatenate(
        (
            jnp.where(upper_side, out_arrived, out_kept),
            jnp.where(upper_side, out_kept, out_arrived),
        ),
        axis=1,
    )


def on_device(
    patches,
    embed_weight,
    embed_bias,
    old_in,
    old_out,
    restore_id,
    norm_gains,
    in_biases,
    out_biases,
    final_gain,
    check_weight,
):
    paired = (
        lax.axis_size("col") == 2
        and old_in.shape[0] % 2 == 0
        and (old_in.shape[0] // 2 * old_in.shape[1]) % lax.axis_size("rep") == 0
    )
    if paired:
        in_weight, out_kept, out_arrived = shared_exchange(old_in, old_out)
    else:
        in_weight, out_weight = butterfly_weights(old_in, old_out)
    layer_gain = pick_rows(restore_id, norm_gains)
    in_bias = pick_rows(restore_id, in_biases)
    out_bias = pick_rows(restore_id, out_biases)
    embedded = jnp.dot(patches, embed_weight, preferred_element_type=jnp.float32) + embed_bias
    normed = norm_rows(embedded, layer_gain)
    tokens = lax.all_gather(normed, "col", axis=0, tiled=True)
    chunk_rows = tokens.shape[0] // CHUNKS
    pre_shares = []
    for chunk in range(CHUNKS):
        partial_pre = jnp.dot(
            tokens[chunk * chunk_rows : (chunk + 1) * chunk_rows],
            in_weight,
            preferred_element_type=jnp.float32,
        ).astype(jnp.bfloat16)
        pre_shares.append(
            lax.psum_scatter(partial_pre, "row", scatter_dimension=0, tiled=True)
        )
    hidden_chunks = [
        jax.nn.gelu(share.astype(jnp.float32) + in_bias, approximate=False).astype(jnp.bfloat16)
        for share in pre_shares
    ]
    if paired:
        hidden_chunks[0], out_arrived = lax.optimization_barrier((hidden_chunks[0], out_arrived))
        out_weight = join_out(out_kept, out_arrived)
    partial_branch = jnp.concatenate(
        [
            jnp.dot(
                lax.all_gather(hidden, "row", axis=0, tiled=True),
                out_weight,
                preferred_element_type=jnp.float32,
            ).astype(jnp.bfloat16)
            for hidden in hidden_chunks
        ],
        axis=0,
    )
    updated = (
        embedded
        + lax.psum_scatter(partial_branch, "col", scatter_dimension=0, tiled=True).astype(jnp.float32)
        + out_bias
    )
    final_normed = norm_rows(updated, final_gain)
    check_logits = lax.psum(
        jnp.dot(final_normed, check_weight, preferred_element_type=jnp.float32), "row"
    )
    return (in_weight, out_weight, check_logits)


def solution(mesh):
    placed = (
        P(("rep", "col"), None),
        P(None, "row"),
        P("row"),
        P(("row", "col"), None, None),
        P(("row", "col"), None, None),
        P(),
        P(None, "row"),
        P(None, "col"),
        P(None, "row"),
        P("row"),
        P("row", None),
    )
    return jax.shard_map(
        on_device,
        mesh=mesh,
        in_specs=placed,
        out_specs=(P("row", "col"), P("col", "row"), P(("rep", "col"), None)),
        check_vma=False,
    )
```
